128 devices in a mesh: rep: 8 (over z, y_hi), fsdp: 16 (over x, y_lo, core).
Axes of the slice: x: 4, y: 4 (y_hi: 2, y_lo: 2; y = y_hi * 2 + y_lo), z: 4, core: 2. Of those that a mesh axis runs over, the one named last changes fastest.
Arguments:
- activations: bfloat16 [8, 32768, 4096], P('rep', 'fsdp'), may hold values from -6 to 6
- cotangent: bfloat16 [8, 32768, 1024], P('rep', 'fsdp'), may hold values from -0.03125 to 0.03125
- momentum: float32 [8, 4096, 1024], P('rep', 'fsdp'), may hold values from -6 to 6
Outputs:
- momentum_next: float32 [8, 4096, 1024], P('rep', 'fsdp')
- update: float32 [4096, 1024], P('fsdp')
The draws below stay inside these ranges and needn't reach their ends.
All inputs are finite; a program needn't handle non-finite values.
Results may differ from the reference program's by a relative error of at most 0.0021.
Values sent between devices are 32-bit elements; how exact they have to be, the bound alone decides.
A program may use at most 128 MiB of HBM per device.

```python
import jax
import jax.numpy as jnp
from jax import lax

D = 4096
KVW = 1024
TOK_DEV = 2048
CH = 64
BAND = 16
TOKENS = 32768
N_REP = 8
N_FSDP = 16


def levels(own_key, extent, pieces, low, high):
    loudness = 1.0
    for dim, shards_of in pieces:
        draws = jax.random.uniform(jax.random.fold_in(jax.random.fold_in(own_key, 6), dim), (shards_of,), jnp.float32, low / len(pieces), high / len(pieces))
        loudness = loudness * jnp.repeat(jnp.exp(draws), extent[dim] // shards_of).reshape((-1,) + (1,) * (len(extent) - 1 - dim))
    return loudness


def gaussian(key, shape, deviation, bound, pieces=(), kind=jnp.bfloat16):
    entries = jax.random.normal(key, shape, jnp.float32) * deviation
    if len(pieces) > 0:
        entries = levels(key, shape, pieces, -0.22, 0.18) * entries
    return jnp.clip(entries, min=-bound, max=bound).astype(kind)


def setup_inputs(seed: int = 0) -> dict:
    seeds = jax.random.split(jax.random.key(seed), 4)
    return {
        "activations": gaussian(seeds[0], (N_REP, TOKENS, D), 1.0, 6.0, ((0, 8), (1, 16))),
        "cotangent": gaussian(seeds[1], (N_REP, TOKENS, KVW), ((TOK_DEV * N_FSDP) ** -0.5), 0.03125, ((0, 8), (1, 16))),
        "momentum": gaussian(seeds[2], (N_REP, D, KVW), 1.0, 6.0, ((0, 8), (1, 16)), jnp.float32),
    }


momentum_decay = 0.9

def basis_rows(size, keep):
    freq = jnp.arange(keep, dtype=jnp.float32)[:, None]
    point = jnp.arange(size, dtype=jnp.float32)[None, :]
    waves = jnp.cos(jnp.pi * (2.0 * point + 1.0) * freq / (2.0 * size))
    scales = jnp.where(freq == 0.0, jnp.sqrt(1.0 / size), jnp.sqrt(2.0 / size))
    return (waves * scales).astype(jnp.float32)

def bands_of(field, basis):
    rows, width = field.shape
    blocks = field.reshape(rows // CH, CH, width // CH, CH)
    return jnp.einsum('kn,anbm,lm->akbl', basis, blocks, basis, precision=lax.Precision.HIGHEST)

def expand(bands, basis):
    count, _, wide, _ = bands.shape
    blocks = jnp.einsum('kn,akbl,lm->anbm', basis, bands, basis, precision=lax.Precision.HIGHEST)
    return blocks.reshape(count * CH, wide * CH)

def reference(activations, cotangent, momentum):
    basis = basis_rows(CH, BAND)
    nexts = []
    total = jnp.zeros((D, KVW), jnp.float32)
    for replica in range(N_REP):
        values = activations[replica].astype(jnp.float32)
        stat = lax.optimization_barrier(jnp.mean(values * values, axis=-1, keepdims=True))
        normed = (values * lax.rsqrt(stat + 1e-05)).astype(jnp.bfloat16)
        grad = lax.dot_general(normed, cotangent[replica], (((0,), (0,)), ((), ())), preferred_element_type=jnp.float32)
        accumulated = momentum_decay * momentum[replica] + grad
        component = expand(bands_of(accumulated, basis), basis)
        nexts.append(accumulated - component)
        total = total + component
    return (jnp.stack(nexts), total / N_REP)
```

```python
import functools

import jax
import jax.numpy as jnp
import numpy as np
from jax import lax
from jax.experimental import pallas as pl
from jax.experimental.pallas import tpu as pltpu
from jax.sharding import PartitionSpec as P

CH = 64
BAND = 16
momentum_decay = 0.9

TOK = 2048
D = 4096
KV = 1024
FB = 256
NA = 576
NB = KV - NA
HA, HB = NA // 2, NB // 2
HALF = KV // 2
RB = 128
XCH = 8
XR = TOK // XCH
MESH = pl.DeviceIdType.MESH
F32 = jnp.float32
BF16 = jnp.bfloat16
HI = lax.Precision.HIGHEST

OPP, NXP, NXM, OWN = 0, 2, 4, 6
NX = (NXP, NXM)
D2D = 0
XA = 8
XB = 20
YB = 26
YA = 30
RY = 31
RZ = 33
NSEM = 39
THROUGH, DIRECT, COMB = 0, 1, 2


def basis():
    freq = np.arange(BAND, dtype=np.float64)[:, None]
    point = np.arange(CH, dtype=np.float64)[None, :]
    waves = np.cos(np.pi * (2.0 * point + 1.0) * freq / (2.0 * CH))
    return (waves * np.where(freq == 0.0, np.sqrt(1.0 / CH), np.sqrt(2.0 / CH))).astype(np.float32)


def dot(a, b):
    return jnp.dot(a, b, precision=HI, preferred_element_type=F32)


def main_kernel(a_hbm, c_hbm, m_hbm, row_ref, rowt_ref, col_ref, colt_ref, next_ref, sum_ref,
                n, c, ct, m, buf, d2d, ra, rb, yb, ya, bsend, by, bsum, bz,
                send_sem, recv_sem, load_sem):
    rep = lax.axis_index("rep")
    me = lax.axis_index("fsdp")
    x, y, core = me // 4, (me // 2) % 2, me % 2
    z, yh = rep // 2, rep % 2
    partner = me + 1 - 2 * core
    xs = (((x + 1) % 4) * 4 + y * 2 + core, ((x + 3) % 4) * 4 + y * 2 + core)
    yp = x * 4 + (1 - y) * 2 + core
    rep_y = z * 2 + 1 - yh
    rep_z = [((z + i) % 4) * 2 + yh for i in (1, 2, 3)]

    barrier = pltpu.get_barrier_semaphore()
    for who in (partner, *xs, yp):
        pl.semaphore_signal(barrier, inc=1, device_id={"fsdp": who}, device_id_type=MESH)
    for who in (rep_y, *rep_z):
        pl.semaphore_signal(barrier, inc=1, device_id={"rep": who}, device_id_type=MESH)

    load_c = pltpu.make_async_copy(c_hbm, c, load_sem.at[0])
    load_c.start()

    def load_x(i):
        rows = pl.ds(pl.multiple_of(i * XR, XR), XR)
        return pltpu.make_async_copy(a_hbm.at[rows], n.at[rows], load_sem.at[2 + i])

    for i in range(XCH):
        load_x(i).start()
    load_m = pltpu.make_async_copy(m_hbm, m, load_sem.at[1])
    load_m.start()

    load_c.wait()

    @pl.loop(0, TOK // 256)
    def _(i):
        cols = pl.ds(pl.multiple_of(i * 256, 256), 256)
        ct[:, cols] = c[cols, :].T

    @pl.loop(0, XCH)
    def _(i):
        load_x(i).wait()

        @pl.loop(0, XR // RB)
        def _(j):
            rows = pl.ds(pl.multiple_of(i * XR + j * RB, RB), RB)
            squares = jnp.zeros((RB, 128), F32)
            for k in range(D // 128):
                v = n[rows, 128 * k : 128 * k + 128].astype(F32)
                squares = squares + v * v
            stat = jnp.sum(squares, axis=-1, keepdims=True) * (1.0 / D)
            scale = jnp.broadcast_to(lax.rsqrt(stat + 1e-05), (RB, 128))
            for k in range(D // 128):
                v = n[rows, 128 * k : 128 * k + 128].astype(F32)
                n[rows, 128 * k : 128 * k + 128] = (v * scale).astype(BF16)

    pl.semaphore_wait(barrier, 8)

    def remote(src, dst, sem, **where):
        return pltpu.make_async_remote_copy(
            src_ref=src, dst_ref=dst, send_sem=send_sem.at[sem], recv_sem=recv_sem.at[sem],
            device_id=where, device_id_type=MESH)

    def pair(k):
        return remote(buf.at[0, k], d2d.at[k], D2D + k, fsdp=partner)

    def half_a(s):
        return pl.ds(s * HA, HA)

    def half_b(s):
        return pl.ds(NA + s * HB, HB)

    def xa(s, j, kind):
        slot = (OPP if kind == THROUGH else NX[s]) + j
        rows = half_a(1 - s if kind == DIRECT else s)
        return remote(buf.at[1, slot, rows], ra.at[s, j, kind], XA + 6 * s + 3 * j + kind, fsdp=xs[s])

    def xb(s, kind):
        slot = (OPP if kind == THROUGH else NX[s]) + 1
        rows = half_b(1 - s if kind == DIRECT else s)
        return remote(buf.at[1, slot, rows], rb.at[s, kind], XB + 3 * s + kind, fsdp=xs[s])

    def yb_msg(i):
        return remote(buf.at[1, 2 * i, pl.ds(NA, NB)], yb.at[i], YB + i, fsdp=yp)

    def ya_msg():
        return remote(buf.at[1, OWN, pl.ds(0, NA)], ya, YA, fsdp=yp)

    def add(slot, rows, got):
        buf[1, slot, rows, :] = buf[1, slot, rows, :] + got[...]

    def take_xa(s, j, kind):
        xa(s, j, kind).wait_recv()
        slot = (NX[s] if kind == THROUGH else OWN) + j
        add(slot, half_a(1 - s if kind == DIRECT else s), ra.at[s, j, kind])

    def take_xb(s, kind):
        xb(s, kind).wait_recv()
        slot = (NX[s] if kind == THROUGH else OWN) + 1
        add(slot, half_b(1 - s if kind == DIRECT else s), rb.at[s, kind])

    def take_yb(i):
        yb_msg(i).wait_recv()
        add(2 * i + 1, pl.ds(NA, NB), yb.at[i])

    def comb_a(j):
        for s in (0, 1):
            take_xa(s, j, THROUGH)
            xa(s, j, COMB).start()

    @pl.loop(0, 17)
    def _(t):
        k, s = t // 2, t % 2

        @pl.when(t < 16)
        def _():
            i, j = k // 2, k % 2
            to_x = (x + 2 - i + 3 * (i // 2) + 2 * (i // 3)) % 4
            to_y = (y + 1 + j) % 2
            to_core = (core + 1 + s) % 2
            first = pl.multiple_of((to_x * 4 + to_y * 2 + to_core) * FB, FB)
            buf[s, k] = jnp.dot(ct[...], n[:, pl.ds(first, FB)], preferred_element_type=F32)

        @pl.when(jnp.logical_and(t < 16, s == 0))
        def _():
            pair(k).start()

        @pl.when(jnp.logical_and(t > 1, s == 0))
        def _():
            done = k - 1
            pair(done).wait_recv()

            @pl.loop(0, KV // 128)
            def _(i):
                rows = pl.ds(pl.multiple_of(i * 128, 128), 128)
                buf[1, done, rows, :] = buf[1, done, rows, :] + d2d[done, rows, :]

            @pl.when(done == 0)
            def _():
                for s in (0, 1):
                    xa(s, 0, THROUGH).start()
                yb_msg(0).start()

            @pl.when(done == 1)
            def _():
                for s in (0, 1):
                    xa(s, 1, THROUGH).start()

            @pl.when(done == 2)
            def _():
                xa(0, 0, DIRECT).start()
                yb_msg(1).start()

            @pl.when(done == 4)
            def _():
                xa(1, 0, DIRECT).start()
                yb_msg(2).start()
                comb_a(0)

            @pl.when(done == 5)
            def _():
                for s in (0, 1):
                    xa(s, 1, DIRECT).start()
                comb_a(1)
                take_yb(0)
                for s in (0, 1):
                    xb(s, THROUGH).start()

    take_yb(1)
    xb(0, DIRECT).start()
    for s in (0, 1):
        take_xa(s, 0, DIRECT)
    for s in (0, 1):
        take_xa(s, 0, COMB)
    ya_msg().start()
    yb_msg(3).start()
    take_yb(2)
    xb(1, DIRECT).start()
    for s in (0, 1):
        take_xa(s, 1, DIRECT)
    for s in (0, 1):
        take_xa(s, 1, COMB)

    load_m.wait()

    def to_y_rep(h):
        return remote(bsend.at[h], by.at[h], RY + h, rep=rep_y)

    def to_z_rep(h, i):
        return remote(bsum.at[h], bz.at[h, i], RZ + 3 * h + i, rep=rep_z[i])

    def finish(h):
        cols = slice(HALF * h, HALF * (h + 1))
        acc = momentum_decay * m[:, cols] + buf[1, OWN + 1, cols, :].T
        next_ref[:, cols] = acc
        bsend[h] = dot(dot(row_ref[...], acc), col_ref[...])
        to_y_rep(h).start()

    def clear(h):
        cols = slice(HALF * h, HALF * (h + 1))
        low = dot(dot(rowt_ref[...], bsend[h]), colt_ref[...])
        next_ref[:, cols] = next_ref[:, cols] - low

    def rep_y_take(h):
        to_y_rep(h).wait_recv()
        bsum[h] = bsend[h] + by[h]
        for i in range(3):
            to_z_rep(h, i).start()

    def rep_z_take(h):
        for i in range(3):
            to_z_rep(h, i).wait_recv()
        sum_ref[:, 128 * h : 128 * (h + 1)] = (bsum[h] + bz[h, 1]) + (bz[h, 0] + bz[h, 2])

    for s in (0, 1):
        take_xb(s, THROUGH)
        xb(s, COMB).start()
    ya_msg().wait_recv()
    add(OWN + 1, pl.ds(0, NA), ya)
    finish(0)
    clear(0)
    rep_y_take(0)
    for s in (0, 1):
        take_xb(s, DIRECT)
    take_yb(3)
    rep_z_take(0)
    for s in (0, 1):
        take_xb(s, COMB)
    finish(1)
    clear(1)
    rep_y_take(1)
    rep_z_take(1)

    for k in range(8):
        pair(k).wait_send()
    for s in (0, 1):
        for kind in range(3):
            for j in (0, 1):
                xa(s, j, kind).wait_send()
            xb(s, kind).wait_send()
    for i in range(4):
        yb_msg(i).wait_send()
    ya_msg().wait_send()
    for h in (0, 1):
        to_y_rep(h).wait_send()
        for i in range(3):
            to_z_rep(h, i).wait_send()


def out_kernel(next_in, sum_ref, rowt_ref, colt_ref, next_out, update_ref):
    next_out[...] = next_in[...]
    for h in (0, 1):
        part = sum_ref[:, 128 * h : 128 * (h + 1)] * 0.125
        update_ref[:, HALF * h : HALF * (h + 1)] = dot(dot(rowt_ref[...], part), colt_ref[...])


def vmem():
    return pl.BlockSpec(memory_space=pltpu.VMEM)


def body(activations, cotangent, momentum):
    base = basis()
    row = np.kron(np.eye(FB // CH, dtype=np.float32), base)
    colt = np.kron(np.eye(HALF // CH, dtype=np.float32), base)
    row, rowt = jnp.asarray(row), jnp.asarray(np.ascontiguousarray(row.T))
    colt, col = jnp.asarray(colt), jnp.asarray(np.ascontiguousarray(colt.T))
    any_space = pl.BlockSpec(memory_space=pl.ANY)
    nb = 4 * BAND
    cleared, summed = pl.pallas_call(
        main_kernel,
        name="step",
        out_shape=(jax.ShapeDtypeStruct((FB, KV), F32), jax.ShapeDtypeStruct((nb, 256), F32)),
        in_specs=[any_space] * 3 + [vmem()] * 4,
        out_specs=(vmem(), vmem()),
        scratch_shapes=[
            pltpu.VMEM((TOK, D), BF16),
            pltpu.VMEM((TOK, KV), BF16),
            pltpu.VMEM((KV, TOK), BF16),
            pltpu.VMEM((FB, KV), F32),
            pltpu.VMEM((2, 8, KV, FB), F32),
            pltpu.VMEM((8, KV, FB), F32),
            pltpu.VMEM((2, 2, 3, HA, FB), F32),
            pltpu.VMEM((2, 3, HB, FB), F32),
            pltpu.VMEM((4, NB, FB), F32),
            pltpu.VMEM((NA, FB), F32),
            pltpu.VMEM((2, nb, 128), F32),
            pltpu.VMEM((2, nb, 128), F32),
            pltpu.VMEM((2, nb, 128), F32),
            pltpu.VMEM((2, 3, nb, 128), F32),
            pltpu.SemaphoreType.DMA((NSEM,)),
            pltpu.SemaphoreType.DMA((NSEM,)),
            pltpu.SemaphoreType.DMA((2 + XCH,)),
        ],
        compiler_params=pltpu.CompilerParams(
            collective_id=0, has_side_effects=True, vmem_limit_bytes=64 * 1024 * 1024 - 256 * 1024),
    )(activations[0], cotangent[0], momentum[0], row, rowt, col, colt)
    cleared, update = pl.pallas_call(
        out_kernel,
        name="outputs",
        out_shape=(jax.ShapeDtypeStruct((FB, KV), F32), jax.ShapeDtypeStruct((FB, KV), F32)),
        in_specs=[vmem()] * 4,
        out_specs=(vmem(), vmem()),
    )(cleared, summed, rowt, colt)
    return cleared[None], update


def solution(mesh):
    return jax.shard_map(
        body,
        mesh=mesh,
        in_specs=(P("rep", "fsdp", None), P("rep", "fsdp", None), P("rep", "fsdp", None)),
        out_specs=(P("rep", "fsdp", None), P("fsdp", None)),
        check_vma=False,
    )
```

```python
import functools

import jax
import jax.numpy as jnp
import numpy as np
from jax import lax
from jax.experimental import pallas as pl
from jax.experimental.pallas import tpu as pltpu
from jax.sharding import PartitionSpec as P

CH = 64
BAND = 16
momentum_decay = 0.9

TOK = 2048
D = 4096
KV = 1024
FB = 256
LOW = KV * BAND // CH
NA = (LOW, 320)
A0 = (0, LOW)
B0 = LOW + NA[1]
NB = KV - B0
HB = NB // 2
XCH = 8
XR = TOK // XCH
RB = 128
MESH = pl.DeviceIdType.MESH
F32 = jnp.float32
BF16 = jnp.bfloat16
HI = lax.Precision.HIGHEST

OWN = 6
D2D = 0
XA = 8
XB = 32
YB = 38
YA = 42
RY = 44
RZ = 45
NSEM = 48
THROUGH, DIRECT, COMB = 0, 1, 2


def basis():
    freq = np.arange(CH, dtype=np.float64)[:, None]
    point = np.arange(CH, dtype=np.float64)[None, :]
    waves = np.cos(np.pi * (2.0 * point + 1.0) * freq / (2.0 * CH))
    return waves * np.where(freq == 0.0, np.sqrt(1.0 / CH), np.sqrt(2.0 / CH))


def dot(a, b):
    return jnp.dot(a, b, precision=HI, preferred_element_type=F32)


def main_kernel(a_hbm, c_hbm, m_hbm, wave_ref, low_ref, lowt_ref, high_ref, next_ref, update_ref,
                n, c, ct, m, buf, d2d, ral, rah, rb, yb, yal, yah, mband, glow, bsend, by, bsum, bz,
                send_sem, recv_sem, load_sem):
    rep = lax.axis_index("rep")
    me = lax.axis_index("fsdp")
    x, y, core = me // 4, (me // 2) % 2, me % 2
    z, yh = rep // 2, rep % 2
    partner = me + 1 - 2 * core
    xs = (((x + 1) % 4) * 4 + y * 2 + core, ((x + 3) % 4) * 4 + y * 2 + core)
    yp = x * 4 + (1 - y) * 2 + core
    rep_y = z * 2 + 1 - yh
    rep_z = [((z + i) % 4) * 2 + yh for i in (1, 2, 3)]

    barrier = pltpu.get_barrier_semaphore()
    for who in (partner, *xs, yp):
        pl.semaphore_signal(barrier, inc=1, device_id={"fsdp": who}, device_id_type=MESH)
    for who in (rep_y, *rep_z):
        pl.semaphore_signal(barrier, inc=1, device_id={"rep": who}, device_id_type=MESH)

    load_c = pltpu.make_async_copy(c_hbm, c, load_sem.at[0])
    load_c.start()

    def load_x(i):
        rows = pl.ds(pl.multiple_of(i * XR, XR), XR)
        return pltpu.make_async_copy(a_hbm.at[rows], n.at[rows], load_sem.at[2 + i])

    for i in range(XCH):
        load_x(i).start()
    load_m = pltpu.make_async_copy(m_hbm, m, load_sem.at[1])
    load_m.start()
    load_c.wait()

    @pl.loop(0, XCH)
    def _(i):
        load_x(i).wait()
        tokens = pl.ds(pl.multiple_of(i * XR, XR), XR)
        for g in range(KV // 256):
            part = c[tokens, 256 * g : 256 * g + 256]
            wave = lax.dot_general(wave_ref[0], part, (((1,), (1,)), ((), ())), preferred_element_type=F32)
            wave = wave + lax.dot_general(wave_ref[1], part, (((1,), (1,)), ((), ())), preferred_element_type=F32)
            wave = wave.astype(BF16)
            ct[64 * g : 64 * g + 64, tokens] = wave[:64]
            ct[LOW + 192 * g : LOW + 192 * g + 192, tokens] = wave[64:]
        for j in range(XR // RB):
            rows = pl.ds(pl.multiple_of(i * XR + j * RB, RB), RB)
            squares = jnp.zeros((RB, 128), F32)
            for k in range(D // 128):
                v = n[rows, 128 * k : 128 * k + 128].astype(F32)
                squares = squares + v * v
            stat = jnp.sum(squares, axis=-1, keepdims=True) * (1.0 / D)
            scale = jnp.broadcast_to(lax.rsqrt(stat + 1e-05), (RB, 128))
            for k in range(D // 128):
                v = n[rows, 128 * k : 128 * k + 128].astype(F32)
                n[rows, 128 * k : 128 * k + 128] = (v * scale).astype(BF16)

    pl.semaphore_wait(barrier, 8)

    def remote(src, dst, sem, **where):
        return pltpu.make_async_remote_copy(
            src_ref=src, dst_ref=dst, send_sem=send_sem.at[sem], recv_sem=recv_sem.at[sem],
            device_id=where, device_id_type=MESH)

    def pair(k):
        return remote(buf.at[0, k], d2d.at[k], D2D + k, fsdp=partner)

    ra = (ral, rah)
    ya = (yal, yah)

    def half_a(p, s):
        return pl.ds(A0[p] + s * (NA[p] // 2), NA[p] // 2)

    def half_b(s):
        return pl.ds(B0 + s * HB, HB)

    def xa(p, s, j, kind):
        slot = 3 * j + (0 if kind == THROUGH else 1 + s)
        rows = half_a(p, 1 - s if kind == DIRECT else s)
        return remote(buf.at[1, slot, rows], ra[p].at[s, j, kind], XA + 12 * p + 6 * s + 3 * j + kind, fsdp=xs[s])

    def xb(s, kind):
        slot = 3 + (0 if kind == THROUGH else 1 + s)
        rows = half_b(1 - s if kind == DIRECT else s)
        return remote(buf.at[1, slot, rows], rb.at[s, kind], XB + 3 * s + kind, fsdp=xs[s])

    def yb_msg(i):
        return remote(buf.at[1, i if i < 3 else OWN, pl.ds(B0, NB)], yb.at[i], YB + i, fsdp=yp)

    def ya_msg(p):
        return remote(buf.at[1, OWN, pl.ds(A0[p], NA[p])], ya[p], YA + p, fsdp=yp)

    def add(slot, rows, got):
        buf[1, slot, rows, :] = buf[1, slot, rows, :] + got[...]

    def start_xa(p, j, kind):
        for s in (0, 1):
            xa(p, s, j, kind).start()

    def take_xa(p, j, kind):
        for s in (0, 1):
            xa(p, s, j, kind).wait_recv()
            slot = 3 * j + 1 + s if kind == THROUGH else OWN + j
            add(slot, half_a(p, 1 - s if kind == DIRECT else s), ra[p].at[s, j, kind])

    def comb_a(p, j):
        take_xa(p, j, THROUGH)
        start_xa(p, j, COMB)

    def take_xb(s, kind):
        xb(s, kind).wait_recv()
        slot = 3 + 1 + s if kind == THROUGH else OWN + 1
        add(slot, half_b(1 - s if kind == DIRECT else s), rb.at[s, kind])

    def take_yb(i):
        yb_msg(i).wait_recv()
        add(3 + i if i < 3 else OWN + 1, pl.ds(B0, NB), yb.at[i])

    def take_ya(p):
        ya_msg(p).wait_recv()
        add(OWN + 1, pl.ds(A0[p], NA[p]), ya[p])

    @pl.loop(0, 17)
    def _(t):
        k, s = t // 2, t % 2

        @pl.when(t < 16)
        def _():
            own = k // 6
            i = (1 - own) * (k % 3) + 3 * own
            j = (1 - own) * (k // 3) + own * (k - 6)
            to_x = (x + 2 - i + 3 * (i // 2) + 2 * (i // 3)) % 4
            to_y = (y + 1 + j) % 2
            to_core = (core + 1 + s) % 2
            first = pl.multiple_of((to_x * 4 + to_y * 2 + to_core) * FB, FB)
            buf[s, k] = jnp.dot(ct[...], n[:, pl.ds(first, FB)], preferred_element_type=F32)

        @pl.when(jnp.logical_and(t < 16, s == 0))
        def _():
            pair(k).start()

        @pl.when(jnp.logical_and(t > 1, s == 0))
        def _():
            done = k - 1
            pair(done).wait_recv()

            @pl.loop(0, KV // 128)
            def _(i):
                rows = pl.ds(pl.multiple_of(i * 128, 128), 128)
                buf[1, done, rows, :] = buf[1, done, rows, :] + d2d[done, rows, :]

            @pl.when(done == 0)
            def _():
                start_xa(0, 0, THROUGH)
                yb_msg(0).start()
                start_xa(1, 0, THROUGH)

            @pl.when(done == 1)
            def _():
                xa(0, 0, 0, DIRECT).start()
                yb_msg(1).start()

            @pl.when(done == 2)
            def _():
                xa(0, 1, 0, DIRECT).start()
                comb_a(0, 0)

            @pl.when(done == 3)
            def _():
                start_xa(0, 1, THROUGH)

            @pl.when(done == 4)
            def _():
                xa(0, 0, 1, DIRECT).start()

            @pl.when(done == 5)
            def _():
                xa(0, 1, 1, DIRECT).start()
                start_xa(1, 0, DIRECT)

            @pl.when(done == 6)
            def _():
                take_xa(0, 0, DIRECT)
                take_xa(0, 0, COMB)
                ya_msg(0).start()
                yb_msg(2).start()

    comb_a(0, 1)
    comb_a(1, 0)
    start_xa(1, 1, THROUGH)
    start_xa(1, 1, DIRECT)
    take_yb(0)
    for s in (0, 1):
        xb(s, THROUGH).start()

    def to_y_rep():
        return remote(bsend, by, RY, rep=rep_y)

    def to_z_rep(i):
        return remote(bsum, bz.at[i], RZ + i, rep=rep_z[i])

    load_m.wait()
    low, lowt, high = low_ref[...], lowt_ref[...], high_ref[...]
    rows_low = dot(low, m[...])
    for g in range(4):
        mband[:, 64 * g : 64 * g + 64] = momentum_decay * dot(rows_low[:, 256 * g : 256 * g + 256], lowt)

    take_yb(1)
    xb(0, DIRECT).start()
    take_xa(0, 1, DIRECT)
    take_xa(0, 1, COMB)
    take_ya(0)
    glow[...] = buf[1, OWN + 1, :LOW, :].T
    bsend[...] = mband[...] + dot(low, glow[...])
    to_y_rep().start()

    take_xa(1, 0, DIRECT)
    take_xa(1, 0, COMB)
    ya_msg(1).start()
    yb_msg(3).start()

    cleared = glow[...] - dot(lowt, bsend[...])
    for g in range(4):
        cols = slice(256 * g, 256 * g + 256)
        next_ref[:, cols] = momentum_decay * m[:, cols] + dot(cleared[:, 64 * g : 64 * g + 64], low)

    comb_a(1, 1)
    take_yb(2)
    xb(1, DIRECT).start()
    to_y_rep().wait_recv()
    bsum[...] = bsend[...] + by[...]
    for i in range(3):
        to_z_rep(i).start()
    for s in (0, 1):
        take_xb(s, THROUGH)
        xb(s, COMB).start()

    def restore(g):
        rows = slice(LOW + 192 * g, LOW + 192 * g + 192)
        cols = slice(256 * g, 256 * g + 256)
        next_ref[:, cols] = next_ref[:, cols] + dot(buf[1, OWN + 1, rows, :].T, high)

    for i in range(3):
        to_z_rep(i).wait_recv()
    bsum_all = ((bsum[...] + bz[1]) + (bz[0] + bz[2])) * 0.125
    wide = dot(lowt, bsum_all)
    for g in range(4):
        update_ref[:, 256 * g : 256 * g + 256] = dot(wide[:, 64 * g : 64 * g + 64], low)

    take_xa(1, 1, DIRECT)
    take_xa(1, 1, COMB)
    take_ya(1)
    restore(0)
    for s in (0, 1):
        take_xb(s, DIRECT)
    take_yb(3)
    for s in (0, 1):
        take_xb(s, COMB)
    for g in (1, 2, 3):
        restore(g)

    for k in range(8):
        pair(k).wait_send()
    for s in (0, 1):
        for kind in range(3):
            for p in (0, 1):
                for j in (0, 1):
                    xa(p, s, j, kind).wait_send()
            xb(s, kind).wait_send()
    for i in range(4):
        yb_msg(i).wait_send()
    for p in (0, 1):
        ya_msg(p).wait_send()
    to_y_rep().wait_send()
    for i in range(3):
        to_z_rep(i).wait_send()


def out_kernel(next_in, update_in, next_out, update_out, sem):
    copies = [pltpu.make_async_copy(src, dst, sem.at[i])
              for i, (src, dst) in enumerate(((next_in, next_out), (update_in, update_out)))]
    for copy in copies:
        copy.start()
    for copy in copies:
        copy.wait()


def vmem():
    return pl.BlockSpec(memory_space=pltpu.VMEM)


def body(activations, cotangent, momentum):
    base = basis()
    blocks = np.eye(FB // CH)
    low = np.kron(blocks, base[:BAND])
    high = np.kron(blocks, base[BAND:])
    wave = np.concatenate([low, high]).astype(np.float32)
    coarse = wave.astype(BF16)
    wave = np.stack([coarse, (wave - coarse.astype(np.float32)).astype(BF16)])
    low, high = low.astype(np.float32), high.astype(np.float32)
    any_space = pl.BlockSpec(memory_space=pl.ANY)
    nb = 4 * BAND
    whole = jax.ShapeDtypeStruct((FB, KV), F32)
    cleared, update = pl.pallas_call(
        main_kernel,
        name="step",
        out_shape=(whole, whole),
        in_specs=[any_space] * 3 + [vmem()] * 4,
        out_specs=(vmem(), vmem()),
        scratch_shapes=[
            pltpu.VMEM((TOK, D), BF16),
            pltpu.VMEM((TOK, KV), BF16),
            pltpu.VMEM((KV, TOK), BF16),
            pltpu.VMEM((FB, KV), F32),
            pltpu.VMEM((2, 8, KV, FB), F32),
            pltpu.VMEM((8, KV, FB), F32),
            pltpu.VMEM((2, 2, 3, NA[0] // 2, FB), F32),
            pltpu.VMEM((2, 2, 3, NA[1] // 2, FB), F32),
            pltpu.VMEM((2, 3, HB, FB), F32),
            pltpu.VMEM((4, NB, FB), F32),
            pltpu.VMEM((NA[0], FB), F32),
            pltpu.VMEM((NA[1], FB), F32),
            pltpu.VMEM((nb, LOW), F32),
            pltpu.VMEM((FB, LOW), F32),
            pltpu.VMEM((nb, LOW), F32),
            pltpu.VMEM((nb, LOW), F32),
            pltpu.VMEM((nb, LOW), F32),
            pltpu.VMEM((3, nb, LOW), F32),
            pltpu.SemaphoreType.DMA((NSEM,)),
            pltpu.SemaphoreType.DMA((NSEM,)),
            pltpu.SemaphoreType.DMA((2 + XCH,)),
        ],
        compiler_params=pltpu.CompilerParams(
            collective_id=0, has_side_effects=True, vmem_limit_bytes=64 * 1024 * 1024 - 256 * 1024),
    )(activations[0], cotangent[0], momentum[0], jnp.asarray(wave), jnp.asarray(low),
      jnp.asarray(np.ascontiguousarray(low.T)), jnp.asarray(high))
    cleared, update = pl.pallas_call(
        out_kernel,
        name="outputs",
        out_shape=(whole, whole),
        in_specs=[vmem(), vmem()],
        out_specs=(any_space, any_space),
        scratch_shapes=[pltpu.SemaphoreType.DMA((2,))],
    )(cleared, update)
    return cleared[None], update


def solution(mesh):
    return jax.shard_map(
        body,
        mesh=mesh,
        in_specs=(P("rep", "fsdp", None), P("rep", "fsdp", None), P("rep", "fsdp", None)),
        out_specs=(P("rep", "fsdp", None), P("fsdp", None)),
        check_vma=False,
    )
```

```python
import functools

import jax
import jax.numpy as jnp
import numpy as np
from jax import lax
from jax.experimental import pallas as pl
from jax.experimental.pallas import tpu as pltpu
from jax.sharding import PartitionSpec as P

CH = 64
BAND = 16
momentum_decay = 0.9

TOK = 2048
D = 4096
KV = 1024
FB = 256
LOW = KV * BAND // CH
NA = (LOW, 320)
A0 = (0, LOW)
B0 = LOW + NA[1]
NB = KV - B0
HB = NB // 2
XCH = 8
XR = TOK // XCH
RB = 64
MESH = pl.DeviceIdType.MESH
F32 = jnp.float32
BF16 = jnp.bfloat16
HI = lax.Precision.HIGHEST

OWN = 6
D2D = 0
XA = 8
XB = 32
YB = 38
YA = 42
RY = 44
RZ = 45
NSEM = 48
THROUGH, DIRECT, COMB = 0, 1, 2


def basis():
    freq = np.arange(CH, dtype=np.float64)[:, None]
    point = np.arange(CH, dtype=np.float64)[None, :]
    waves = np.cos(np.pi * (2.0 * point + 1.0) * freq / (2.0 * CH))
    return waves * np.where(freq == 0.0, np.sqrt(1.0 / CH), np.sqrt(2.0 / CH))


def dot(a, b):
    return jnp.dot(a, b, precision=HI, preferred_element_type=F32)


def main_kernel(a_hbm, c_hbm, m_hbm, wave_ref, low_ref, lowt_ref, high_ref, next_hbm, update_hbm,
                next_ref, update_ref, n, c, ct, m, buf, d2d, ral, rah, rb, yb, yal, yah, mband, glow, bsend, by, bsum, bz,
                send_sem, recv_sem, load_sem, out_sem):
    rep = lax.axis_index("rep")
    me = lax.axis_index("fsdp")
    x, y, core = me // 4, (me // 2) % 2, me % 2
    z, yh = rep // 2, rep % 2
    partner = me + 1 - 2 * core
    xs = (((x + 1) % 4) * 4 + y * 2 + core, ((x + 3) % 4) * 4 + y * 2 + core)
    yp = x * 4 + (1 - y) * 2 + core
    rep_y = z * 2 + 1 - yh
    rep_z = [((z + i) % 4) * 2 + yh for i in (1, 2, 3)]

    barrier = pltpu.get_barrier_semaphore()
    for who in (partner, *xs, yp):
        pl.semaphore_signal(barrier, inc=1, device_id={"fsdp": who}, device_id_type=MESH)
    for who in (rep_y, *rep_z):
        pl.semaphore_signal(barrier, inc=1, device_id={"rep": who}, device_id_type=MESH)

    load_c = pltpu.make_async_copy(c_hbm, c, load_sem.at[0])
    load_c.start()

    def load_x(i):
        rows = pl.ds(pl.multiple_of(i * XR, XR), XR)
        return pltpu.make_async_copy(a_hbm.at[rows], n.at[rows], load_sem.at[2 + i])

    for i in range(XCH):
        load_x(i).start()
    load_m = pltpu.make_async_copy(m_hbm, m, load_sem.at[1])
    load_m.start()
    load_c.wait()

    @pl.loop(0, XCH)
    def _(i):
        load_x(i).wait()
        tokens = pl.ds(pl.multiple_of(i * XR, XR), XR)
        for g in range(KV // 256):
            part = c[tokens, 256 * g : 256 * g + 256]
            wave = lax.dot_general(wave_ref[0], part, (((1,), (1,)), ((), ())), preferred_element_type=F32)
            wave = wave + lax.dot_general(wave_ref[1], part, (((1,), (1,)), ((), ())), preferred_element_type=F32)
            wave = wave.astype(BF16)
            ct[64 * g : 64 * g + 64, tokens] = wave[:64]
            ct[LOW + 192 * g : LOW + 192 * g + 192, tokens] = wave[64:]
        for j in range(XR // RB):
            rows = pl.ds(pl.multiple_of(i * XR + j * RB, RB), RB)
            squares = jnp.zeros((RB, 128), F32)
            for k in range(D // 128):
                v = n[rows, 128 * k : 128 * k + 128].astype(F32)
                squares = squares + v * v
            stat = jnp.sum(squares, axis=-1, keepdims=True) * (1.0 / D)
            scale = jnp.broadcast_to(lax.rsqrt(stat + 1e-05), (RB, 128))
            for k in range(D // 128):
                v = n[rows, 128 * k : 128 * k + 128].astype(F32)
                n[rows, 128 * k : 128 * k + 128] = (v * scale).astype(BF16)

    pl.semaphore_wait(barrier, 8)

    def remote(src, dst, sem, **where):
        return pltpu.make_async_remote_copy(
            src_ref=src, dst_ref=dst, send_sem=send_sem.at[sem], recv_sem=recv_sem.at[sem],
            device_id=where, device_id_type=MESH)

    def pair(k):
        return remote(buf.at[0, k], d2d.at[k], D2D + k, fsdp=partner)

    ra = (ral, rah)
    ya = (yal, yah)

    def half_a(p, s):
        return pl.ds(A0[p] + s * (NA[p] // 2), NA[p] // 2)

    def half_b(s):
        return pl.ds(B0 + s * HB, HB)

    def xa(p, s, j, kind):
        slot = 3 * j + (0 if kind == THROUGH else 1 + s)
        rows = half_a(p, 1 - s if kind == DIRECT else s)
        return remote(buf.at[1, slot, rows], ra[p].at[s, j, kind], XA + 12 * p + 6 * s + 3 * j + kind, fsdp=xs[s])

    def xb(s, kind):
        slot = 3 + (0 if kind == THROUGH else 1 + s)
        rows = half_b(1 - s if kind == DIRECT else s)
        return remote(buf.at[1, slot, rows], rb.at[s, kind], XB + 3 * s + kind, fsdp=xs[s])

    def yb_msg(i):
        return remote(buf.at[1, i if i < 3 else OWN, pl.ds(B0, NB)], yb.at[i], YB + i, fsdp=yp)

    def ya_msg(p):
        return remote(buf.at[1, OWN, pl.ds(A0[p], NA[p])], ya[p], YA + p, fsdp=yp)

    def add(slot, rows, got):
        buf[1, slot, rows, :] = buf[1, slot, rows, :] + got[...]

    def start_xa(p, j, kind):
        for s in (0, 1):
            xa(p, s, j, kind).start()

    def take_xa(p, j, kind):
        for s in (0, 1):
            xa(p, s, j, kind).wait_recv()
            slot = 3 * j + 1 + s if kind == THROUGH else OWN + j
            add(slot, half_a(p, 1 - s if kind == DIRECT else s), ra[p].at[s, j, kind])

    def comb_a(p, j):
        take_xa(p, j, THROUGH)
        start_xa(p, j, COMB)

    def take_xb(s, kind):
        xb(s, kind).wait_recv()
        slot = 3 + 1 + s if kind == THROUGH else OWN + 1
        add(slot, half_b(1 - s if kind == DIRECT else s), rb.at[s, kind])

    def take_yb(i):
        yb_msg(i).wait_recv()
        add(3 + i if i < 3 else OWN + 1, pl.ds(B0, NB), yb.at[i])

    def take_ya(p):
        ya_msg(p).wait_recv()
        add(OWN + 1, pl.ds(A0[p], NA[p]), ya[p])

    @pl.loop(0, 17)
    def _(t):
        k, s = t // 2, t % 2

        @pl.when(t < 16)
        def _():
            own = k // 6
            i = (1 - own) * (k % 3) + 3 * own
            j = (1 - own) * (k // 3) + own * (k - 6)
            to_x = (x + 2 - i + 3 * (i // 2) + 2 * (i // 3)) % 4
            to_y = (y + 1 + j) % 2
            to_core = (core + 1 + s) % 2
            first = pl.multiple_of((to_x * 4 + to_y * 2 + to_core) * FB, FB)
            buf[s, k] = jnp.dot(ct[...], n[:, pl.ds(first, FB)], preferred_element_type=F32)

        @pl.when(jnp.logical_and(t < 16, s == 0))
        def _():
            pair(k).start()

        @pl.when(jnp.logical_and(t > 1, s == 0))
        def _():
            done = k - 1
            pair(done).wait_recv()

            @pl.loop(0, KV // 128)
            def _(i):
                rows = pl.ds(pl.multiple_of(i * 128, 128), 128)
                buf[1, done, rows, :] = buf[1, done, rows, :] + d2d[done, rows, :]

            @pl.when(done == 0)
            def _():
                start_xa(0, 0, THROUGH)
                yb_msg(0).start()
                start_xa(1, 0, THROUGH)

            @pl.when(done == 1)
            def _():
                xa(0, 0, 0, DIRECT).start()
                yb_msg(1).start()

            @pl.when(done == 2)
            def _():
                xa(0, 1, 0, DIRECT).start()
                comb_a(0, 0)

            @pl.when(done == 3)
            def _():
                start_xa(0, 1, THROUGH)

            @pl.when(done == 4)
            def _():
                xa(0, 0, 1, DIRECT).start()

            @pl.when(done == 5)
            def _():
                xa(0, 1, 1, DIRECT).start()
                start_xa(1, 0, DIRECT)

            @pl.when(done == 6)
            def _():
                take_xa(0, 0, DIRECT)
                take_xa(0, 0, COMB)
                ya_msg(0).start()
                yb_msg(2).start()

    comb_a(0, 1)
    comb_a(1, 0)
    start_xa(1, 1, THROUGH)
    start_xa(1, 1, DIRECT)
    take_yb(0)
    for s in (0, 1):
        xb(s, THROUGH).start()

    def to_y_rep():
        return remote(bsend, by, RY, rep=rep_y)

    def to_z_rep(i):
        return remote(bsum, bz.at[i], RZ + i, rep=rep_z[i])

    load_m.wait()
    low, lowt, high = low_ref[...], lowt_ref[...], high_ref[...]
    rows_low = dot(low, m[...])
    for g in range(4):
        mband[:, 64 * g : 64 * g + 64] = momentum_decay * dot(rows_low[:, 256 * g : 256 * g + 256], lowt)

    take_yb(1)
    xb(0, DIRECT).start()
    take_xa(0, 1, DIRECT)
    take_xa(0, 1, COMB)
    take_ya(0)
    glow[...] = buf[1, OWN + 1, :LOW, :].T
    bsend[...] = mband[...] + dot(low, glow[...])
    to_y_rep().start()

    take_xa(1, 0, DIRECT)
    take_xa(1, 0, COMB)
    ya_msg(1).start()
    yb_msg(3).start()

    cleared = glow[...] - dot(lowt, bsend[...])
    for g in range(4):
        cols = slice(256 * g, 256 * g + 256)
        next_ref[:, cols] = momentum_decay * m[:, cols] + dot(cleared[:, 64 * g : 64 * g + 64], low)

    comb_a(1, 1)
    take_yb(2)
    xb(1, DIRECT).start()
    to_y_rep().wait_recv()
    bsum[...] = bsend[...] + by[...]
    for i in range(3):
        to_z_rep(i).start()
    for s in (0, 1):
        take_xb(s, THROUGH)
        xb(s, COMB).start()

    def restore(g):
        rows = slice(LOW + 192 * g, LOW + 192 * g + 192)
        cols = slice(256 * g, 256 * g + 256)
        next_ref[:, cols] = next_ref[:, cols] + dot(buf[1, OWN + 1, rows, :].T, high)

    def put(g):
        cols = pl.ds(256 * g, 256)
        return pltpu.make_async_copy(next_ref.at[:, cols], next_hbm.at[:, cols], out_sem.at[g])

    put_update = pltpu.make_async_copy(update_ref, update_hbm, out_sem.at[4])
    for i in range(3):
        to_z_rep(i).wait_recv()
    bsum_all = ((bsum[...] + bz[1]) + (bz[0] + bz[2])) * 0.125
    wide = dot(lowt, bsum_all)
    for g in range(4):
        update_ref[:, 256 * g : 256 * g + 256] = dot(wide[:, 64 * g : 64 * g + 64], low)
    put_update.start()

    take_xa(1, 1, DIRECT)
    take_xa(1, 1, COMB)
    take_ya(1)
    restore(0)
    put(0).start()
    for s in (0, 1):
        take_xb(s, DIRECT)
    take_yb(3)
    for s in (0, 1):
        take_xb(s, COMB)
    for g in (1, 2, 3):
        restore(g)
        put(g).start()
    put_update.wait()
    for g in range(4):
        put(g).wait()

    for k in range(8):
        pair(k).wait_send()
    for s in (0, 1):
        for kind in range(3):
            for p in (0, 1):
                for j in (0, 1):
                    xa(p, s, j, kind).wait_send()
            xb(s, kind).wait_send()
    for i in range(4):
        yb_msg(i).wait_send()
    for p in (0, 1):
        ya_msg(p).wait_send()
    to_y_rep().wait_send()
    for i in range(3):
        to_z_rep(i).wait_send()


def out_kernel(next_in, update_in, next_out, update_out, held, get_sem, put_sem):
    pieces = 4
    rows = FB // pieces
    gets, puts = [], []
    for i, (src, dst) in enumerate(((update_in, update_out), (next_in, next_out))):
        for j in range(pieces):
            at = pl.ds(j * rows, rows)
            sem = i * pieces + j
            gets.append(pltpu.make_async_copy(src.at[at], held.at[i, at], get_sem.at[sem]))
            puts.append(pltpu.make_async_copy(held.at[i, at], dst.at[at], put_sem.at[sem]))
    for get in gets:
        get.start()
    for get, put in zip(gets, puts):
        get.wait()
        put.start()
    for put in puts:
        put.wait()


def vmem():
    return pl.BlockSpec(memory_space=pltpu.VMEM)


def body(activations, cotangent, momentum):
    base = basis()
    blocks = np.eye(FB // CH)
    low = np.kron(blocks, base[:BAND])
    high = np.kron(blocks, base[BAND:])
    wave = np.concatenate([low, high]).astype(np.float32)
    coarse = wave.astype(BF16)
    wave = np.stack([coarse, (wave - coarse.astype(np.float32)).astype(BF16)])
    low, high = low.astype(np.float32), high.astype(np.float32)
    any_space = pl.BlockSpec(memory_space=pl.ANY)
    nb = 4 * BAND
    whole = jax.ShapeDtypeStruct((FB, KV), F32)
    cleared, update = pl.pallas_call(
        main_kernel,
        name="step",
        out_shape=(whole, whole),
        in_specs=[any_space] * 3 + [vmem()] * 4,
        out_specs=(any_space, any_space),
        scratch_shapes=[
            pltpu.VMEM((FB, KV), F32),
            pltpu.VMEM((FB, KV), F32),
            pltpu.VMEM((TOK, D), BF16),
            pltpu.VMEM((TOK, KV), BF16),
            pltpu.VMEM((KV, TOK), BF16),
            pltpu.VMEM((FB, KV), F32),
            pltpu.VMEM((2, 8, KV, FB), F32),
            pltpu.VMEM((8, KV, FB), F32),
            pltpu.VMEM((2, 2, 3, NA[0] // 2, FB), F32),
            pltpu.VMEM((2, 2, 3, NA[1] // 2, FB), F32),
            pltpu.VMEM((2, 3, HB, FB), F32),
            pltpu.VMEM((4, NB, FB), F32),
            pltpu.VMEM((NA[0], FB), F32),
            pltpu.VMEM((NA[1], FB), F32),
            pltpu.VMEM((nb, LOW), F32),
            pltpu.VMEM((FB, LOW), F32),
            pltpu.VMEM((nb, LOW), F32),
            pltpu.VMEM((nb, LOW), F32),
            pltpu.VMEM((nb, LOW), F32),
            pltpu.VMEM((3, nb, LOW), F32),
            pltpu.SemaphoreType.DMA((NSEM,)),
            pltpu.SemaphoreType.DMA((NSEM,)),
            pltpu.SemaphoreType.DMA((2 + XCH,)),
            pltpu.SemaphoreType.DMA((5,)),
        ],
        compiler_params=pltpu.CompilerParams(
            collective_id=0, has_side_effects=True, vmem_limit_bytes=64 * 1024 * 1024 - 256 * 1024),
    )(activations[0], cotangent[0], momentum[0], jnp.asarray(wave), jnp.asarray(low),
      jnp.asarray(np.ascontiguousarray(low.T)), jnp.asarray(high))
    cleared, update = pl.pallas_call(
        out_kernel,
        name="outputs",
        out_shape=(whole, whole),
        in_specs=[any_space, any_space],
        out_specs=(any_space, any_space),
        scratch_shapes=[
            pltpu.VMEM((2, FB, KV), F32),
            pltpu.SemaphoreType.DMA((8,)),
            pltpu.SemaphoreType.DMA((8,)),
        ],
    )(cleared, update)
    return cleared[None], update


def solution(mesh):
    return jax.shard_map(
        body,
        mesh=mesh,
        in_specs=(P("rep", "fsdp", None), P("rep", "fsdp", None), P("rep", "fsdp", None)),
        out_specs=(P("rep", "fsdp", None), P("fsdp", None)),
        check_vma=False,
    )
```
